32 devices in a mesh: between: 4 (over y, core), inside: 8 (over z, x).
Axes of the slice: x: 2, y: 2, z: 4, core: 2. Of those that a mesh axis runs over, the one named last changes fastest.
Arguments:
- inputs: bfloat16 [16384, 4096], P(('between', 'inside')), may hold values from -6 to 6
- grad_out: bfloat16 [16384, 1024], P(('between', 'inside')), may hold values from -6 to 6
- error: float32 [4, 4096, 1024], P('between', 'inside'), may hold values from -4 to 4
- momentum: float32 [4096, 1024], P('inside'), may hold values from -4 to 4
- weight: bfloat16 [4096, 1024], P('inside'), may hold values from -6 to 6
- tile_index: int32 [4, 8, 4, 32], P('between', 'inside'), may hold values from -1 to 1023, as said below
Outputs:
- new_weight: bfloat16 [4096, 1024], replicated
- new_momentum: float32 [4096, 1024], P('inside')
- new_error: float32 [4, 4096, 1024], P('between', 'inside')
The draws below stay inside these ranges and needn't reach their ends.
Inputs may be any that keep to these rules, and one draw needn't show every extreme that they name: `tile_index`: for each island, device and owning island the live entries are distinct and stand first, the rest are -1; their number varies strongly from block to block, and in every draw some device and owner have all 32 slots live on all 4 islands.
All inputs are finite; a program needn't handle non-finite values.
Results may differ from the reference program's by a relative error of at most 0.0035.
Values may be sent and summed in bfloat16 or wider, within the bound.
No kernel may reach another device: no remote copies, remote signals or barrier semaphores. Data moves between devices by JAX's collectives and lax.ppermute only.
A program may use at most 128 MiB of HBM per device.

```python
import math
import jax
import jax.numpy as jnp
from jax import lax

FEAT = 4096
KV = 1024
TILE = 128
CAP = 32
TOK_DEV = 512
ISLANDS = 4
TOKENS = 16384
TILES_ROW = 8
OWN_TILES = 1024
N_BETWEEN = 4
N_INSIDE = 8


def draw_tile_index(key, part):
    key_order = jax.random.fold_in(key, 11)
    key_count = jax.random.fold_in(key, 12)
    key_device = jax.random.fold_in(key, 13)
    key_owner = jax.random.fold_in(key, 14)
    shape = (N_BETWEEN, N_INSIDE, N_BETWEEN)
    scores = jax.random.randint(key_order, shape + (OWN_TILES,), 0, 1 << 20) * OWN_TILES + jnp.arange(OWN_TILES, dtype=jnp.int32)
    order = jnp.argsort(scores, axis=-1, stable=True).astype(jnp.int32)[..., :CAP]
    shifts = jax.random.randint(key_count, shape, 0, 4)
    counts = jnp.maximum(jnp.right_shift(jnp.full(shape, CAP, jnp.int32), shifts), 1)
    device_full = jax.random.randint(key_device, (), 0, N_INSIDE)
    owner_full = jax.random.randint(key_owner, (), 0, N_BETWEEN)
    device_ids = jnp.arange(N_INSIDE, dtype=jnp.int32)[None, :, None]
    owner_ids = jnp.arange(N_BETWEEN, dtype=jnp.int32)[None, None, :]
    full = jnp.logical_and(device_ids == device_full, owner_ids == owner_full)
    counts = jnp.where(full, CAP, counts)
    slots = jnp.arange(CAP, dtype=jnp.int32)
    return jnp.where(slots < counts[..., None], order, -1).astype(jnp.int32)


def raised(values, rng, source, target, shards_of, factor):
    def block_of(position):
        return (jnp.arange(values.shape[position]) // (values.shape[position] // shards_of)).reshape((-1,) + (1,) * (values.ndim - 1 - position))

    first = jax.random.permutation(rng, shards_of)[block_of(target)]
    far = (block_of(target) + shards_of // 2) % shards_of
    return jnp.where((block_of(source) == first) | (block_of(source) == far), factor * values, values)


def shard_levels(stream_key, shape, cuts, low, top_value):
    factor_of = 1.0
    for axis_at, parts in cuts:
        steps = jax.random.uniform(jax.random.fold_in(jax.random.fold_in(stream_key, 6), axis_at), (parts,), jnp.float32, low / len(cuts), top_value / len(cuts))
        factor_of = factor_of * jnp.repeat(jnp.exp(steps), shape[axis_at] // parts).reshape((-1,) + (1,) * (len(shape) - 1 - axis_at))
    return factor_of


def normal_values(own_key, dims, deviation, most, split=(), kind=jnp.bfloat16):
    array = jax.random.normal(own_key, dims, jnp.float32) * deviation
    if len(split) > 0:
        array = shard_levels(own_key, dims, split, -0.22, 0.18) * array
    return jnp.clip(array, min=-most, max=most).astype(kind)


def gaussian_with(rng, dims, spread, most, pieces, heavy, kind=jnp.bfloat16):
    entries = spread * jax.random.normal(rng, dims, jnp.float32)
    if pieces:
        entries = entries * shard_levels(rng, dims, pieces, -0.22, 0.18)
    return jnp.clip(raised(entries, jax.random.fold_in(rng, 3), *heavy), -most, most).astype(kind)


def setup_inputs(seed: int = 0) -> dict:
    key_list = jax.random.split(jax.random.key(seed), 7)
    return {
        "inputs": gaussian_with(key_list[0], (TOKENS, FEAT), 1.0, 6.0, ((0, 32),), (0, 1, 32, 2.75)),
        "grad_out": normal_values(key_list[1], (TOKENS, KV), 1.0, 6.0, ((0, 32),)),
        "error": normal_values(key_list[2], (ISLANDS, FEAT, KV), 0.5, 4.0, ((0, 4), (1, 8)), jnp.float32),
        "momentum": normal_values(key_list[3], (FEAT, KV), 0.5, 4.0, ((0, 8),), jnp.float32),
        "weight": normal_values(key_list[4], (FEAT, KV), 1.0, 6.0, ((0, 8),)),
        "tile_index": draw_tile_index(jax.random.fold_in(key_list[6], 71), 0),
    }


feedback_decay = 0.95
outer_rate = 0.7
outer_momentum = 0.9

def island_grad(x_island, dy_island):

    def add_term(total, pair):
        term = jnp.dot(pair[0].T, pair[1], preferred_element_type=jnp.float32)
        return (total + term, None)
    total, _ = lax.scan(add_term, jnp.zeros((FEAT, KV), jnp.float32), (x_island, dy_island))
    return total

def reference(inputs, grad_out, error, momentum, weight, tile_index):
    islands = N_BETWEEN
    group = N_INSIDE
    x_all = inputs.reshape(islands, group, TOK_DEV, FEAT)
    dy_all = grad_out.reshape(islands, group, TOK_DEV, KV)
    scale = 1.0 / math.sqrt(TOK_DEV * group)
    grads = jnp.stack([island_grad(x_all[b], dy_all[b]) for b in range(islands)])
    accum = feedback_decay * error + scale * grads
    hit = jnp.any(tile_index[..., None] == jnp.arange(OWN_TILES, dtype=jnp.int32), axis=3)
    mask = jnp.repeat(hit.reshape(islands, FEAT, TILES_ROW), TILE, axis=2)
    sent = jnp.where(mask, accum, 0.0).astype(jnp.bfloat16)
    new_error = jnp.where(mask, 0.0, accum)
    delta = lax.optimization_barrier(jnp.sum(sent.astype(jnp.float32), axis=0)) / islands
    new_momentum = outer_momentum * momentum + delta
    new_weight = (weight.astype(jnp.float32) - outer_rate * (delta + outer_momentum * new_momentum)).astype(jnp.bfloat16)
    return (new_weight, new_momentum, new_error)
```

```python
import math

import jax
import jax.numpy as jnp
from jax import lax
from jax.experimental import pallas as pl
from jax.experimental.pallas import tpu as pltpu
from jax.sharding import PartitionSpec as P


TILE = 128


feedback_decay = 0.95
outer_rate = 0.7
outer_momentum = 0.9


def swap(values, axis, bit):
    size = lax.axis_size(axis)
    return lax.ppermute(values, axis, [(i, i ^ (1 << bit)) for i in range(size)])


def spread(values):
    size = lax.axis_size("inside")
    every = jnp.broadcast_to(values[None], (size, *values.shape))
    return lax.all_to_all(every, "inside", split_axis=0, concat_axis=0, tiled=True)


def swap_sets(sets, bit):
    out = []
    for one in sets:
        out.append([])
        for values in one:
            out[-1].append(swap(values, "between", bit))
    return out


def dot_t(left, right):
    return lax.dot_general(left, right, (((0,), (0,)), ((), ())), preferred_element_type=jnp.float32)


def take_halves(place, x, rows_dev, chunks, first, count):
    tokens, feat = x.shape
    halves = feat // rows_dev // 2
    rows = rows_dev // chunks

    def column(k):
        return lambda h, p: (0, (2 * h + 1 - p[0]) * chunks + k)

    def body(place_ref, *refs):
        for k in range(count):
            refs[count + k][...] = refs[k][...]

    return pl.pallas_call(
        body,
        grid_spec=pltpu.PrefetchScalarGridSpec(
            num_scalar_prefetch=1,
            grid=(halves,),
            in_specs=[pl.BlockSpec((tokens, rows), column(first + k)) for k in range(count)],
            out_specs=[pl.BlockSpec((tokens, rows), lambda h, p: (0, h)) for _ in range(count)],
        ),
        out_shape=[jax.ShapeDtypeStruct((tokens, halves * rows), x.dtype) for _ in range(count)],
        name="take_halves",
    )(place, *([x] * count))


def pair_dot(place, x_own, x_recv, dy_own, dy_recv, chunk, chunks, halves):
    tokens, width = dy_own.shape
    rows = x_recv.shape[1] // halves
    quarter = halves // 2
    steps = 2
    columns = width // steps

    def own_spec(i, mine):
        def at(c, p):
            half = 2 * i + (p[1] if mine else 1 - p[1])
            return (0, (2 * half + p[0]) * chunks + chunk)

        return pl.BlockSpec((tokens, rows), at)

    def body(p, *refs):
        owns, (xr, do, dr, send, keep) = refs[: 2 * quarter], refs[2 * quarter :]
        recvs = []
        for mine in (False, True):
            for i in range(quarter):
                half = 2 * i + (p[1] if mine else 1 - p[1])
                recvs.append(xr[:, pl.ds(pl.multiple_of(half * rows, rows), rows)])
        own = jnp.concatenate([r[...] for r in owns], axis=1)
        recv = jnp.concatenate(recvs, axis=1)
        total = dot_t(own, do[...]) + dot_t(recv, dr[...])
        total = total.reshape(2, quarter, rows, columns)
        send[...] = total[0].astype(send.dtype)
        keep[...] = total[1]

    return pl.pallas_call(
        body,
        grid_spec=pltpu.PrefetchScalarGridSpec(
            num_scalar_prefetch=1,
            grid=(steps,),
            in_specs=[
                *[own_spec(i, mine) for mine in (False, True) for i in range(quarter)],
                pl.BlockSpec((tokens, halves * rows), lambda c, p: (0, 0)),
                pl.BlockSpec((tokens, columns), lambda c, p: (0, c)),
                pl.BlockSpec((tokens, columns), lambda c, p: (0, c)),
            ],
            out_specs=[pl.BlockSpec((quarter, rows, columns), lambda c, p: (0, 0, c))] * 2,
        ),
        out_shape=[
            jax.ShapeDtypeStruct((quarter, rows, width), jnp.bfloat16),
            jax.ShapeDtypeStruct((quarter, rows, width), jnp.float32),
        ],
        name="pair_dot",
    )(place, *([x_own] * (2 * quarter)), x_recv, dy_own, dy_recv)


def slot_terms(place, x, dy, index, rows_dev, own_rows):
    tokens, width = dy.shape
    tiles_row = width // TILE
    group, _, slots = index.shape
    cap = slots * own_rows // rows_dev

    def body(p, ix, xb, dyb, out, flipped):
        @pl.when(pl.program_id(0) == 0)
        def _():
            flipped[...] = dyb[...].T

        picked = []
        for side in range(2):
            at = jnp.maximum(ix[side], 0)
            owner = lax.broadcasted_iota(jnp.int32, (1, slots), 1) // cap
            row = owner * own_rows + at // tiles_row
            onehot = jnp.where(lax.broadcasted_iota(jnp.int32, (rows_dev, slots), 0) == row, 1.0, 0.0).astype(jnp.bfloat16)
            picked.append(jnp.dot(xb[:, side * rows_dev : (side + 1) * rows_dev], onehot, preferred_element_type=jnp.float32).astype(jnp.bfloat16))
        terms = jnp.dot(flipped[...], jnp.concatenate(picked, axis=1), preferred_element_type=jnp.float32)
        for side in range(2):
            column = jnp.maximum(ix[side], 0) % tiles_row
            total = jnp.zeros((TILE, slots), jnp.float32)
            for c in range(tiles_row):
                total = jnp.where(column == c, terms[c * TILE : (c + 1) * TILE, side * slots : (side + 1) * slots], total)
            out[side] = total.T.astype(jnp.bfloat16)

    return pl.pallas_call(
        body,
        grid_spec=pltpu.PrefetchScalarGridSpec(
            num_scalar_prefetch=1,
            grid=(group // 2,),
            in_specs=[
                pl.BlockSpec((2, 1, slots), lambda i, p: (i, 0, 0)),
                pl.BlockSpec((tokens, 2 * rows_dev), lambda i, p: (0, i)),
                pl.BlockSpec((tokens, width), lambda i, p: (0, 0)),
            ],
            out_specs=pl.BlockSpec((2, slots, TILE), lambda i, p: (i, 0, 0)),
            scratch_shapes=[pltpu.VMEM((width, tokens), jnp.bfloat16)],
        ),
        out_shape=jax.ShapeDtypeStruct((group, slots, TILE), jnp.bfloat16),
        name="slot_terms",
    )(place, index, x, dy)


def block_delta(ix, values, own_rows, tiles_row):
    slots = ix.shape[1]
    q = lax.broadcasted_iota(jnp.int32, (own_rows, slots), 0) * tiles_row
    onehot = [jnp.where(q == ix - c, 1.0, 0.0).astype(jnp.bfloat16) for c in range(tiles_row)]
    return jnp.dot(jnp.concatenate(onehot, axis=0), values, preferred_element_type=jnp.float32)


def momentum_step(place, momentum, index, values):
    rows_dev, width = momentum.shape
    islands, _, owners, cap, _ = values.shape
    own_rows = rows_dev // owners
    tiles_row = width // TILE
    slots = islands * cap

    def body(p, ix, v, mom, out):
        parts = block_delta(ix[0, 0], v[...].reshape(slots, TILE), own_rows, tiles_row)
        for c in range(tiles_row):
            at = slice(c * TILE, (c + 1) * TILE)
            part = parts[c * own_rows : (c + 1) * own_rows]
            out[:, at] = outer_momentum * mom[:, at] + part * (1.0 / islands)

    return pl.pallas_call(
        body,
        grid_spec=pltpu.PrefetchScalarGridSpec(
            num_scalar_prefetch=1,
            grid=(owners,),
            in_specs=[
                pl.BlockSpec((1, 1, 1, slots), lambda o, p: (p[2], o, 0, 0)),
                pl.BlockSpec((islands, 1, 1, cap, TILE), lambda o, p: (0, p[2], o, 0, 0)),
                pl.BlockSpec((own_rows, width), lambda o, p: (o, 0)),
            ],
            out_specs=pl.BlockSpec((own_rows, width), lambda o, p: (o, 0)),
        ),
        out_shape=jax.ShapeDtypeStruct(momentum.shape, jnp.float32),
        name="momentum_step",
    )(place, index, values, momentum)


def weight_step(sets, groups, where, index, values, shape, before=None):
    count, subs = len(sets), len(sets[0])
    per = sets[0][0].shape[0]
    pieces = subs * per
    halves, _, islands, own_rows, width = shape
    cap = values.shape[3]
    tiles_row = width // TILE
    slots = islands * cap
    rate = outer_rate * (1.0 + outer_momentum) / islands
    flat = [a for one in sets for a in one]

    def body(w, ix, v, *refs):
        arrays, (out, held, sems) = refs[: len(flat)], refs[-3:]
        step = pl.program_id(0)

        def copy(n):
            to = held.at[n // subs, pl.ds(n % subs * per, per)]
            return pltpu.make_async_copy(arrays[n], to, sems.at[n])

        @pl.when(step == 0)
        def _():
            for n in range(len(flat)):
                copy(n).start()

        for s in range(count):

            @pl.when(step == s)
            def _(s=s):
                for u in range(subs):
                    copy(s * subs + u).wait()

        owner = w[2 + step]
        for i in range(pieces):
            device = w[1] ^ groups[i]
            parts = block_delta(ix[device, owner], v[:, device, owner].reshape(slots, TILE), own_rows, tiles_row)
            to = device >> 1
            for c in range(tiles_row):
                at = slice(c * TILE, (c + 1) * TILE)
                part = parts[c * own_rows : (c + 1) * own_rows]
                out[to, 0, 0, :, at] = (held[step, i, :, at].astype(jnp.float32) - rate * part).astype(jnp.bfloat16)

    extra = [] if before is None else [before]
    return pl.pallas_call(
        body,
        grid_spec=pltpu.PrefetchScalarGridSpec(
            num_scalar_prefetch=1,
            grid=(count,),
            in_specs=[
                pl.BlockSpec(index.shape, lambda g, w: (0, 0, 0, 0)),
                pl.BlockSpec(values.shape, lambda g, w: (0, 0, 0, 0, 0)),
                *[pl.BlockSpec(memory_space=pl.ANY) for _ in flat + extra],
            ],
            out_specs=pl.BlockSpec((halves, 1, 1, own_rows, width), lambda g, w: (0, w[0], w[2 + g], 0, 0)),
            scratch_shapes=[
                pltpu.VMEM((count, pieces, own_rows, width), jnp.bfloat16),
                pltpu.SemaphoreType.DMA((len(flat),)),
            ],
        ),
        out_shape=jax.ShapeDtypeStruct(shape, jnp.bfloat16),
        input_output_aliases={} if before is None else {3 + len(flat): 0},
        name="weight_step",
    )(where, index, values, *flat, *extra)


def local(inputs, grad_out, error, momentum, weight, tile_index):
    group = lax.axis_size("inside")
    islands = lax.axis_size("between")
    tokens, feat = inputs.shape
    width = grad_out.shape[1]
    rows_dev = feat // group
    own_rows = rows_dev // islands
    tiles_row = width // TILE
    own_tiles = own_rows * tiles_row
    cap = tile_index.shape[3]
    inside_bits = group.bit_length() - 1
    outer_bits = [*range(1, islands.bit_length() - 1), 0]
    chunks = max(1, min(4, rows_dev // TILE))
    rows = rows_dev // chunks
    halves = group // 2
    j = lax.axis_index("inside")
    b = lax.axis_index("between")
    place = jnp.stack([j & 1, (j >> 1) & 1, j])
    index = tile_index[0, 0]

    numbers = spread(index)
    island_numbers = numbers.reshape(group, 1, islands * cap)

    dy_recv = swap(grad_out, "inside", 0)
    x_send = take_halves(place, inputs, rows_dev, chunks, 0, 1)
    if chunks > 1:
        x_send += take_halves(place, inputs, rows_dev, chunks, 1, chunks - 1)

    terms = slot_terms(place, inputs, grad_out, island_numbers, rows_dev, own_rows)
    index, terms, numbers = lax.optimization_barrier((index, terms, numbers))
    terms = lax.all_to_all(terms, "inside", split_axis=0, concat_axis=0, tiled=True)

    numbers = numbers[None]
    for bit in outer_bits:
        numbers = jnp.concatenate([numbers, swap(numbers, "between", bit)], axis=0)
    by_device = numbers.transpose(1, 2, 0, 3).reshape(group, islands, 1, islands * cap)

    start = b * own_rows
    base = (
        lax.dynamic_slice_in_dim(weight, start, own_rows, 0).astype(jnp.float32)
        - outer_rate * outer_momentum * outer_momentum * lax.dynamic_slice_in_dim(momentum, start, own_rows, 0)
    ).astype(jnp.bfloat16)[None]
    base_parts = []
    base_group = [0]
    for bit in reversed(range(1, inside_bits)):
        last = swap(base, "inside", bit)
        base_parts = [base, last]
        base = jnp.concatenate(base_parts, axis=0)
        base_group += [g ^ (1 << bit) for g in base_group]

    x_recv = []
    for k in range(chunks):
        x_recv.append(swap(x_send[k], "inside", 0))

    scale = 1.0 / math.sqrt(tokens * group)
    tiles = error[0].reshape(islands, own_tiles, TILE)
    picked = jnp.take_along_axis(tiles, jnp.maximum(index, 0)[:, :, None], axis=1)
    sums = jnp.sum(terms.astype(jnp.float32), axis=0).reshape(islands, cap, TILE)
    sent = jnp.where(index[:, :, None] >= 0, feedback_decay * picked + scale * sums, 0.0).astype(jnp.bfloat16)
    values = spread(sent)[None]
    for bit in outer_bits:
        values = jnp.concatenate([values, swap(values, "between", bit)], axis=0)

    across = []
    for part in base_parts:
        across.append(swap(part, "inside", 0))
    near_sets, far_sets = [[base]], [across]
    owners = [0]
    for bit in outer_bits:
        near_sets += swap_sets(near_sets, bit)
        far_sets += swap_sets(far_sets, bit)
        owners += [o ^ (1 << bit) for o in owners]
    set_owner = [b ^ o for o in owners]
    new_weight = None
    for parity, sets in enumerate((near_sets, far_sets)):
        gone = [g ^ parity for g in base_group]
        where = jnp.stack([(j & 1) ^ parity, j, *set_owner])
        new_weight = weight_step(
            sets, gone, where, by_device, values,
            (halves, 2, islands, own_rows, width), new_weight,
        )
    new_weight = new_weight.reshape(feat, width)
    new_momentum = momentum_step(place, momentum, by_device, values)

    hit = jnp.any(index[:, None, None, :] == jnp.arange(own_tiles, dtype=jnp.int32).reshape(1, own_rows, tiles_row, 1), axis=3)
    free = jnp.where(hit.reshape(rows_dev, tiles_row, 1), 0.0, 1.0)
    free = jnp.broadcast_to(free, (rows_dev, tiles_row, TILE)).reshape(rows_dev, width)
    parts = []
    for k in range(chunks):
        send, keep = pair_dot(place, inputs, x_recv[k], grad_out, dy_recv, k, chunks, halves)
        current = keep + swap(send, "inside", 1).astype(jnp.float32)
        for bit in range(2, inside_bits):
            mine = (j >> bit) & 1
            current = current.reshape(current.shape[0] // 2, 2, rows, width)
            send = lax.dynamic_index_in_dim(current, 1 - mine, 1, keepdims=False).astype(jnp.bfloat16)
            keep = lax.dynamic_index_in_dim(current, mine, 1, keepdims=False)
            current = keep + swap(send, "inside", bit).astype(jnp.float32)
        parts.append(current[0])
    grad = jnp.concatenate(parts, axis=0)
    new_error = (free * (feedback_decay * error[0] + scale * grad))[None]
    return (new_weight, new_momentum, new_error)


def solution(mesh):
    in_specs = (
        P(("between", "inside"), None),
        P(("between", "inside"), None),
        P("between", "inside", None),
        P("inside", None),
        P("inside", None),
        P("between", "inside", None, None),
    )
    out_specs = (P(), P("inside", None), P("between", "inside", None))
    return jax.shard_map(local, mesh=mesh, in_specs=in_specs, out_specs=out_specs, check_vma=False)
```

```python
import math

import jax
import jax.numpy as jnp
from jax import lax
from jax.experimental import pallas as pl
from jax.experimental.pallas import tpu as pltpu
from jax.sharding import PartitionSpec as P


TILE = 128


feedback_decay = 0.95
outer_rate = 0.7
outer_momentum = 0.9


def swap(values, axis, bit):
    size = lax.axis_size(axis)
    return lax.ppermute(values, axis, [(i, i ^ (1 << bit)) for i in range(size)])


def spread(values):
    size = lax.axis_size("inside")
    every = jnp.broadcast_to(values[None], (size, *values.shape))
    return lax.all_to_all(every, "inside", split_axis=0, concat_axis=0, tiled=True)


def swap_sets(sets, bit):
    out = []
    for one in sets:
        out.append([])
        for values in one:
            out[-1].append(swap(values, "between", bit))
    return out


def take_halves(place, x, rows_dev, chunks):
    tokens, feat = x.shape
    halves = feat // rows_dev // 2
    rows = rows_dev // chunks

    def body(p, xb, *outs):
        for k in range(chunks):
            outs[k][...] = xb[:, k * rows : (k + 1) * rows]

    return pl.pallas_call(
        body,
        grid_spec=pltpu.PrefetchScalarGridSpec(
            num_scalar_prefetch=1,
            grid=(halves,),
            in_specs=[pl.BlockSpec((tokens, rows_dev), lambda h, p: (0, 2 * h + 1 - p[0]))],
            out_specs=[pl.BlockSpec((tokens, rows), lambda h, p: (0, h)) for _ in range(chunks)],
        ),
        out_shape=[jax.ShapeDtypeStruct((tokens, halves * rows), x.dtype) for _ in range(chunks)],
        name="take_halves",
    )(place, x)


def pair_dot(place, x_own, x_recv, dy_own, dy_recv, chunk, chunks, halves):
    tokens, width = dy_own.shape
    rows = x_recv.shape[1] // halves
    quarter = halves // 2
    steps = 2
    columns = width // steps

    def own_spec(i, mine):
        def at(c, p):
            half = 2 * i + (p[1] if mine else 1 - p[1])
            return (0, (2 * half + p[0]) * chunks + chunk)

        return pl.BlockSpec((tokens, rows), at)

    def body(p, *refs):
        owns, (xr, do, dr, send, keep, own, recv) = refs[: 2 * quarter], refs[2 * quarter :]

        @pl.when(pl.program_id(0) == 0)
        def _():
            n = 0
            for mine in (False, True):
                for i in range(quarter):
                    half = 2 * i + (p[1] if mine else 1 - p[1])
                    at = slice(n * rows, (n + 1) * rows)
                    own[at] = owns[n][...].T
                    recv[at] = xr[:, pl.ds(pl.multiple_of(half * rows, rows), rows)].T
                    n += 1

        total = jnp.dot(own[...], do[...], preferred_element_type=jnp.float32)
        total = total + jnp.dot(recv[...], dr[...], preferred_element_type=jnp.float32)
        total = total.reshape(2, quarter, rows, columns)
        send[...] = total[0].astype(send.dtype)
        keep[...] = total[1]

    return pl.pallas_call(
        body,
        grid_spec=pltpu.PrefetchScalarGridSpec(
            num_scalar_prefetch=1,
            grid=(steps,),
            in_specs=[
                *[own_spec(i, mine) for mine in (False, True) for i in range(quarter)],
                pl.BlockSpec((tokens, halves * rows), lambda c, p: (0, 0)),
                pl.BlockSpec((tokens, columns), lambda c, p: (0, c)),
                pl.BlockSpec((tokens, columns), lambda c, p: (0, c)),
            ],
            out_specs=[pl.BlockSpec((quarter, rows, columns), lambda c, p: (0, 0, c))] * 2,
            scratch_shapes=[pltpu.VMEM((2 * quarter * rows, tokens), jnp.bfloat16)] * 2,
        ),
        out_shape=[
            jax.ShapeDtypeStruct((quarter, rows, width), jnp.bfloat16),
            jax.ShapeDtypeStruct((quarter, rows, width), jnp.float32),
        ],
        name="pair_dot",
    )(place, *([x_own] * (2 * quarter)), x_recv, dy_own, dy_recv)


def slot_terms(place, x, dy, index, rows_dev, own_rows):
    tokens, width = dy.shape
    tiles_row = width // TILE
    group, _, slots = index.shape
    cap = slots * own_rows // rows_dev

    def body(p, ix, xb, dyb, out, flipped):
        @pl.when(pl.program_id(0) == 0)
        def _():
            flipped[...] = dyb[...].T

        picked = []
        for side in range(2):
            at = jnp.maximum(ix[side], 0)
            owner = lax.broadcasted_iota(jnp.int32, (1, slots), 1) // cap
            row = owner * own_rows + at // tiles_row
            onehot = jnp.where(lax.broadcasted_iota(jnp.int32, (rows_dev, slots), 0) == row, 1.0, 0.0).astype(jnp.bfloat16)
            picked.append(jnp.dot(xb[:, side * rows_dev : (side + 1) * rows_dev], onehot, preferred_element_type=jnp.float32).astype(jnp.bfloat16))
        terms = jnp.dot(flipped[...], jnp.concatenate(picked, axis=1), preferred_element_type=jnp.float32)
        for side in range(2):
            column = jnp.maximum(ix[side], 0) % tiles_row
            total = jnp.zeros((TILE, slots), jnp.float32)
            for c in range(tiles_row):
                total = jnp.where(column == c, terms[c * TILE : (c + 1) * TILE, side * slots : (side + 1) * slots], total)
            out[side] = total.T.astype(jnp.bfloat16)

    return pl.pallas_call(
        body,
        grid_spec=pltpu.PrefetchScalarGridSpec(
            num_scalar_prefetch=1,
            grid=(group // 2,),
            in_specs=[
                pl.BlockSpec((2, 1, slots), lambda i, p: (i, 0, 0)),
                pl.BlockSpec((tokens, 2 * rows_dev), lambda i, p: (0, i)),
                pl.BlockSpec((tokens, width), lambda i, p: (0, 0)),
            ],
            out_specs=pl.BlockSpec((2, slots, TILE), lambda i, p: (i, 0, 0)),
            scratch_shapes=[pltpu.VMEM((width, tokens), jnp.bfloat16)],
        ),
        out_shape=jax.ShapeDtypeStruct((group, slots, TILE), jnp.bfloat16),
        name="slot_terms",
    )(place, index, x, dy)


def block_onehot(ix, own_rows, tiles_row, live=None):
    slots = ix.shape[1]
    kind = jnp.bfloat16 if own_rows <= 256 else jnp.float32
    q = lax.broadcasted_iota(jnp.int32, (own_rows, slots), 0).astype(jnp.float32).astype(kind)
    named = ix >= 0 if live is None else jnp.logical_and(ix >= 0, live)
    row = jnp.maximum(ix, 0) // tiles_row
    column = jnp.maximum(ix, 0) - row * tiles_row
    out = []
    for c in range(tiles_row):
        at = jnp.where(jnp.logical_and(named, column == c), row, -1).astype(jnp.float32).astype(kind)
        out.append(jnp.where(q == at, jnp.ones((), kind), jnp.zeros((), kind)).astype(jnp.bfloat16))
    return jnp.concatenate(out, axis=0)


def block_delta(ix, values, own_rows, tiles_row):
    return jnp.dot(block_onehot(ix, own_rows, tiles_row), values, preferred_element_type=jnp.float32)


def error_step(place, parts, first, index, error, own_rows, scale, before):
    rows_dev, width = error.shape
    count, each = len(parts), len(parts[0])
    rows = parts[0][0].shape[1]
    group = 4 * parts[0][0].shape[0]
    tiles_row = width // TILE
    owners = rows_dev // own_rows
    slots = index.shape[1]
    cap = slots // owners
    flat = [a for part in parts for a in part]

    def body(p, ix, err, *refs):
        out = refs[-1]
        lane = lax.broadcasted_iota(jnp.int32, (1, slots), 1) // cap
        for s in range(count):

            @pl.when(pl.program_id(0) == s)
            def _(s=s):
                terms = refs[s * each : (s + 1) * each]
                for n in range(rows // own_rows):
                    owner = (first + s) * (rows // own_rows) + n
                    onehot = block_onehot(ix[...], own_rows, tiles_row, lane == owner)
                    hits = jnp.dot(onehot, jnp.ones((slots, TILE), jnp.bfloat16), preferred_element_type=jnp.float32)
                    to = slice(n * own_rows, (n + 1) * own_rows)
                    for c in range(tiles_row):
                        at = slice(c * TILE, (c + 1) * TILE)
                        grad = terms[0][0, to, at]
                        for term in terms[1:]:
                            grad = grad + term[0, to, at].astype(jnp.float32)
                        value = feedback_decay * err[to, at] + scale * grad
                        out[to, at] = jnp.where(hits[c * own_rows : (c + 1) * own_rows] > 0.0, 0.0, value)

    def own_block(a):
        shift = (group // a.shape[0]).bit_length() - 1
        return pl.BlockSpec((1, rows, width), lambda g, p: (p[2] >> shift, 0, 0))

    extra = [] if before is None else [before]
    block = pl.BlockSpec((rows, width), lambda g, p: (first + g, 0))
    return pl.pallas_call(
        body,
        grid_spec=pltpu.PrefetchScalarGridSpec(
            num_scalar_prefetch=1,
            grid=(count,),
            in_specs=[
                pl.BlockSpec(index.shape, lambda g, p: (0, 0)), block, *[own_block(a) for a in flat],
                *[pl.BlockSpec(memory_space=pl.ANY) for _ in extra],
            ],
            out_specs=block,
        ),
        out_shape=jax.ShapeDtypeStruct(error.shape, jnp.float32),
        input_output_aliases={} if before is None else {3 + len(flat): 0},
        name="error_step",
    )(place, index, error, *flat, *extra)


def weight_step(sets, groups, where, index, values, shape, momentum=None, before=None):
    count, subs = len(sets), len(sets[0])
    per = sets[0][0].shape[0]
    pieces = subs * per
    halves, _, islands, own_rows, width = shape
    cap = values.shape[3]
    tiles_row = width // TILE
    slots = islands * cap
    rate = outer_rate * (1.0 + outer_momentum) / islands
    flat = [a for one in sets for a in one]

    def body(w, ix, v, *refs):
        arrays, (held, sems) = refs[: len(flat)], refs[-2:]
        out = refs[-3] if momentum is None else refs[-4]
        step = pl.program_id(0)

        def copy(n):
            to = held.at[n // subs, pl.ds(n % subs * per, per)]
            return pltpu.make_async_copy(arrays[n], to, sems.at[n])

        @pl.when(step == 0)
        def _():
            for n in range(len(flat)):
                copy(n).start()

        for s in range(count):

            @pl.when(step == s)
            def _(s=s):
                for u in range(subs):
                    copy(s * subs + u).wait()

        owner = w[2 + step]
        for i in range(pieces):
            device = w[1] ^ groups[i]
            parts = block_delta(ix[device, owner], v[:, device, owner].reshape(slots, TILE), own_rows, tiles_row)
            to = device >> 1
            for c in range(tiles_row):
                at = slice(c * TILE, (c + 1) * TILE)
                part = parts[c * own_rows : (c + 1) * own_rows]
                if momentum is not None and groups[i] == 0:
                    refs[-3][:, at] = outer_momentum * refs[len(flat)][:, at] + part * (1.0 / islands)
                out[to, 0, 0, :, at] = (held[step, i, :, at].astype(jnp.float32) - rate * part).astype(jnp.bfloat16)

    extra = [v for v in (momentum, before) if v is not None]
    rows = pl.BlockSpec((own_rows, width), lambda g, w: (w[2 + g], 0))
    hbm = pl.BlockSpec(memory_space=pl.ANY)
    new_weight = jax.ShapeDtypeStruct(shape, jnp.bfloat16)
    block = pl.BlockSpec((halves, 1, 1, own_rows, width), lambda g, w: (0, w[0], w[2 + g], 0, 0))
    return pl.pallas_call(
        body,
        grid_spec=pltpu.PrefetchScalarGridSpec(
            num_scalar_prefetch=1,
            grid=(count,),
            in_specs=[
                pl.BlockSpec(index.shape, lambda g, w: (0, 0, 0, 0)),
                pl.BlockSpec(values.shape, lambda g, w: (0, 0, 0, 0, 0)),
                *[hbm for _ in flat],
                *([] if momentum is None else [rows]),
                *([] if before is None else [hbm]),
            ],
            out_specs=block if momentum is None else [block, rows],
            scratch_shapes=[
                pltpu.VMEM((count, pieces, own_rows, width), jnp.bfloat16),
                pltpu.SemaphoreType.DMA((len(flat),)),
            ],
        ),
        out_shape=new_weight if momentum is None else [new_weight, jax.ShapeDtypeStruct(momentum.shape, jnp.float32)],
        input_output_aliases={} if before is None else {2 + len(flat) + len(extra): 0},
        name="weight_step",
    )(where, index, values, *flat, *extra)


def local(inputs, grad_out, error, momentum, weight, tile_index):
    group = lax.axis_size("inside")
    islands = lax.axis_size("between")
    tokens, feat = inputs.shape
    width = grad_out.shape[1]
    rows_dev = feat // group
    own_rows = rows_dev // islands
    tiles_row = width // TILE
    own_tiles = own_rows * tiles_row
    cap = tile_index.shape[3]
    inside_bits = group.bit_length() - 1
    outer_bits = [*range(1, islands.bit_length() - 1), 0]
    chunks = max(1, min(4, rows_dev // TILE))
    rows = rows_dev // chunks
    halves = group // 2
    j = lax.axis_index("inside")
    b = lax.axis_index("between")
    place = jnp.stack([j & 1, (j >> 1) & 1, j])
    index = tile_index[0, 0]

    numbers = spread(index)
    island_numbers = numbers.reshape(group, 1, islands * cap)

    dy_recv = swap(grad_out, "inside", 0)
    x_send = take_halves(place, inputs, rows_dev, chunks)

    terms = slot_terms(place, inputs, grad_out, island_numbers, rows_dev, own_rows)
    terms, numbers = lax.optimization_barrier((terms, numbers))
    terms = lax.all_to_all(terms, "inside", split_axis=0, concat_axis=0, tiled=True)

    numbers = numbers[None]
    for bit in outer_bits:
        numbers = jnp.concatenate([numbers, swap(numbers, "between", bit)], axis=0)
    by_device = numbers.transpose(1, 2, 0, 3).reshape(group, islands, 1, islands * cap)

    start = b * own_rows
    base = (
        lax.dynamic_slice_in_dim(weight, start, own_rows, 0).astype(jnp.float32)
        - outer_rate * outer_momentum * outer_momentum * lax.dynamic_slice_in_dim(momentum, start, own_rows, 0)
    ).astype(jnp.bfloat16)[None]
    base_parts = []
    base_group = [0]
    for bit in reversed(range(1, inside_bits)):
        last = swap(base, "inside", bit)
        base_parts = [base, last]
        base = jnp.concatenate(base_parts, axis=0)
        base_group += [g ^ (1 << bit) for g in base_group]

    x_recv = []
    for k in range(chunks):
        x_recv.append(swap(x_send[k], "inside", 0))

    scale = 1.0 / math.sqrt(tokens * group)
    tiles = error[0].reshape(islands, own_tiles, TILE)
    picked = jnp.take_along_axis(tiles, jnp.maximum(index, 0)[:, :, None], axis=1)
    sums = jnp.sum(terms.astype(jnp.float32), axis=0).reshape(islands, cap, TILE)
    sent = jnp.where(index[:, :, None] >= 0, feedback_decay * picked + scale * sums, 0.0).astype(jnp.bfloat16)
    values = spread(sent)[None]
    for bit in outer_bits:
        values = jnp.concatenate([values, swap(values, "between", bit)], axis=0)

    across = []
    for part in base_parts:
        across.append(swap(part, "inside", 0))
    near_sets, far_sets = [[base]], [across]
    owners = [0]
    for bit in outer_bits:
        near_sets += swap_sets(near_sets, bit)
        far_sets += swap_sets(far_sets, bit)
        owners += [o ^ (1 << bit) for o in owners]
    set_owner = [b ^ o for o in owners]
    shape = (halves, 2, islands, own_rows, width)
    where = [jnp.stack([(j & 1) ^ parity, j, *set_owner]) for parity in range(2)]
    new_weight, new_momentum = weight_step(near_sets, base_group, where[0], by_device, values, shape, momentum)
    new_weight = weight_step(far_sets, [g ^ 1 for g in base_group], where[1], by_device, values, shape, None, new_weight)
    new_weight = new_weight.reshape(feat, width)

    parts = []
    for k in range(chunks):
        send, keep = pair_dot(place, inputs, x_recv[k], grad_out, dy_recv, k, chunks, halves)
        recv = swap(send, "inside", 1)
        terms = [keep, recv]
        for bit in range(2, inside_bits):
            current = (keep + recv.astype(jnp.float32)).reshape(keep.shape[0] // 2, 2, rows, width)
            mine = (j >> bit) & 1
            send = lax.dynamic_index_in_dim(current, 1 - mine, 1, keepdims=False).astype(jnp.bfloat16)
            keep = lax.dynamic_index_in_dim(current, mine, 1, keepdims=False)
            recv = swap(send, "inside", bit)
            terms.append(recv)
        parts.append(terms)
    flat_index = index.reshape(1, islands * cap)
    new_error = None
    for first, some in ((0, parts[:-1]), (chunks - 1, parts[-1:])):
        if some:
            new_error = error_step(place, some, first, flat_index, error[0], own_rows, scale, new_error)
    new_error = new_error[None]
    return (new_weight, new_momentum, new_error)


def solution(mesh):
    in_specs = (
        P(("between", "inside"), None),
        P(("between", "inside"), None),
        P("between", "inside", None),
        P("inside", None),
        P("inside", None),
        P("between", "inside", None, None),
    )
    out_specs = (P(), P("inside", None), P("between", "inside", None))
    return jax.shard_map(local, mesh=mesh, in_specs=in_specs, out_specs=out_specs, check_vma=False)
```

```python
import math

import jax
import jax.numpy as jnp
from jax import lax
from jax.experimental import pallas as pl
from jax.experimental.pallas import tpu as pltpu
from jax.sharding import PartitionSpec as P


TILE = 128


feedback_decay = 0.95
outer_rate = 0.7
outer_momentum = 0.9


def swap(values, axis, bit):
    size = lax.axis_size(axis)
    return lax.ppermute(values, axis, [(i, i ^ (1 << bit)) for i in range(size)])


def spread(values):
    size = lax.axis_size("inside")
    every = jnp.broadcast_to(values[None], (size, *values.shape))
    return lax.all_to_all(every, "inside", split_axis=0, concat_axis=0, tiled=True)


def swap_sets(sets, bit):
    out = []
    for one in sets:
        out.append([])
        for values in one:
            out[-1].append(swap(values, "between", bit))
    return out


def take_halves(place, x, rows_dev, chunks):
    tokens, feat = x.shape
    halves = feat // rows_dev // 2
    rows = rows_dev // chunks

    def body(p, xb, *outs):
        for k in range(chunks):
            outs[k][...] = xb[:, k * rows : (k + 1) * rows]

    return pl.pallas_call(
        body,
        grid_spec=pltpu.PrefetchScalarGridSpec(
            num_scalar_prefetch=1,
            grid=(halves,),
            in_specs=[pl.BlockSpec((tokens, rows_dev), lambda h, p: (0, 2 * h + 1 - p[0]))],
            out_specs=[pl.BlockSpec((tokens, rows), lambda h, p: (0, h)) for _ in range(chunks)],
        ),
        out_shape=[jax.ShapeDtypeStruct((tokens, halves * rows), x.dtype) for _ in range(chunks)],
        name="take_halves",
    )(place, x)


def pair_dot(place, x_own, x_recv, dy_own, dy_recv, chunk, chunks, halves):
    tokens, width = dy_own.shape
    rows = x_recv.shape[1] // halves
    quarter = halves // 2
    steps = 2
    columns = width // steps

    def own_spec(i, mine):
        def at(c, p):
            half = 2 * i + (p[1] if mine else 1 - p[1])
            return (0, (2 * half + p[0]) * chunks + chunk)

        return pl.BlockSpec((tokens, rows), at)

    def body(p, *refs):
        owns, (xr, do, dr, send, keep, own, recv) = refs[: 2 * quarter], refs[2 * quarter :]

        @pl.when(pl.program_id(0) == 0)
        def _():
            n = 0
            for mine in (False, True):
                for i in range(quarter):
                    half = 2 * i + (p[1] if mine else 1 - p[1])
                    at = slice(n * rows, (n + 1) * rows)
                    own[at] = owns[n][...].T
                    recv[at] = xr[:, pl.ds(pl.multiple_of(half * rows, rows), rows)].T
                    n += 1

        total = jnp.dot(own[...], do[...], preferred_element_type=jnp.float32)
        total = total + jnp.dot(recv[...], dr[...], preferred_element_type=jnp.float32)
        total = total.reshape(2, quarter, rows, columns)
        send[...] = total[0].astype(send.dtype)
        keep[...] = total[1]

    return pl.pallas_call(
        body,
        grid_spec=pltpu.PrefetchScalarGridSpec(
            num_scalar_prefetch=1,
            grid=(steps,),
            in_specs=[
                *[own_spec(i, mine) for mine in (False, True) for i in range(quarter)],
                pl.BlockSpec((tokens, halves * rows), lambda c, p: (0, 0)),
                pl.BlockSpec((tokens, columns), lambda c, p: (0, c)),
                pl.BlockSpec((tokens, columns), lambda c, p: (0, c)),
            ],
            out_specs=[pl.BlockSpec((quarter, rows, columns), lambda c, p: (0, 0, c))] * 2,
            scratch_shapes=[pltpu.VMEM((2 * quarter * rows, tokens), jnp.bfloat16)] * 2,
        ),
        out_shape=[
            jax.ShapeDtypeStruct((quarter, rows, width), jnp.bfloat16),
            jax.ShapeDtypeStruct((quarter, rows, width), jnp.float32),
        ],
        name="pair_dot",
    )(place, *([x_own] * (2 * quarter)), x_recv, dy_own, dy_recv)


def slot_terms(place, x, dy, index, rows_dev, own_rows):
    tokens, width = dy.shape
    tiles_row = width // TILE
    group, _, slots = index.shape
    cap = slots * own_rows // rows_dev

    def body(p, ix, xb, dyb, out, flipped):
        @pl.when(pl.program_id(0) == 0)
        def _():
            flipped[...] = dyb[...].T

        picked = []
        for side in range(2):
            at = jnp.maximum(ix[side], 0)
            owner = lax.broadcasted_iota(jnp.int32, (1, slots), 1) // cap
            row = owner * own_rows + at // tiles_row
            onehot = jnp.where(lax.broadcasted_iota(jnp.int32, (rows_dev, slots), 0) == row, 1.0, 0.0).astype(jnp.bfloat16)
            picked.append(jnp.dot(xb[:, side * rows_dev : (side + 1) * rows_dev], onehot, preferred_element_type=jnp.float32).astype(jnp.bfloat16))
        terms = jnp.dot(flipped[...], jnp.concatenate(picked, axis=1), preferred_element_type=jnp.float32)
        for side in range(2):
            column = jnp.maximum(ix[side], 0) % tiles_row
            total = jnp.zeros((TILE, slots), jnp.float32)
            for c in range(tiles_row):
                total = jnp.where(column == c, terms[c * TILE : (c + 1) * TILE, side * slots : (side + 1) * slots], total)
            out[side] = total.T.astype(jnp.bfloat16)

    return pl.pallas_call(
        body,
        grid_spec=pltpu.PrefetchScalarGridSpec(
            num_scalar_prefetch=1,
            grid=(group // 2,),
            in_specs=[
                pl.BlockSpec((2, 1, slots), lambda i, p: (i, 0, 0)),
                pl.BlockSpec((tokens, 2 * rows_dev), lambda i, p: (0, i)),
                pl.BlockSpec((tokens, width), lambda i, p: (0, 0)),
            ],
            out_specs=pl.BlockSpec((2, slots, TILE), lambda i, p: (i, 0, 0)),
            scratch_shapes=[pltpu.VMEM((width, tokens), jnp.bfloat16)],
        ),
        out_shape=jax.ShapeDtypeStruct((group, slots, TILE), jnp.bfloat16),
        name="slot_terms",
    )(place, index, x, dy)


def block_onehot(ix, own_rows, tiles_row, live=None):
    slots = ix.shape[1]
    kind = jnp.bfloat16 if own_rows <= 256 else jnp.float32
    q = lax.broadcasted_iota(jnp.int32, (own_rows, slots), 0).astype(jnp.float32).astype(kind)
    named = ix >= 0 if live is None else jnp.logical_and(ix >= 0, live)
    row = jnp.maximum(ix, 0) // tiles_row
    column = jnp.maximum(ix, 0) - row * tiles_row
    out = []
    for c in range(tiles_row):
        at = jnp.where(jnp.logical_and(named, column == c), row, -1).astype(jnp.float32).astype(kind)
        out.append(jnp.where(q == at, jnp.ones((), kind), jnp.zeros((), kind)).astype(jnp.bfloat16))
    return jnp.concatenate(out, axis=0)


def block_delta(ix, values, own_rows, tiles_row):
    return jnp.dot(block_onehot(ix, own_rows, tiles_row), values, preferred_element_type=jnp.float32)


def error_step(place, parts, first, index, error, own_rows, scale, before):
    rows_dev, width = error.shape
    count, each = len(parts), len(parts[0])
    rows = parts[0][0].shape[1]
    group = 4 * parts[0][0].shape[0]
    tiles_row = width // TILE
    owners = rows_dev // own_rows
    slots = index.shape[1]
    cap = slots // owners
    flat = [a for part in parts for a in part]

    def body(p, ix, err, *refs):
        out = refs[-1]
        lane = lax.broadcasted_iota(jnp.int32, (1, slots), 1) // cap
        for s in range(count):

            @pl.when(pl.program_id(0) == s)
            def _(s=s):
                terms = refs[s * each : (s + 1) * each]
                for n in range(rows // own_rows):
                    owner = (first + s) * (rows // own_rows) + n
                    onehot = block_onehot(ix[...], own_rows, tiles_row, lane == owner)
                    hits = jnp.dot(onehot, jnp.ones((slots, TILE), jnp.bfloat16), preferred_element_type=jnp.float32)
                    to = slice(n * own_rows, (n + 1) * own_rows)
                    for c in range(tiles_row):
                        at = slice(c * TILE, (c + 1) * TILE)
                        grad = terms[0][0, to, at]
                        for term in terms[1:]:
                            grad = grad + term[0, to, at].astype(jnp.float32)
                        value = feedback_decay * err[to, at] + scale * grad
                        out[to, at] = jnp.where(hits[c * own_rows : (c + 1) * own_rows] > 0.0, 0.0, value)

    def own_block(a):
        shift = (group // a.shape[0]).bit_length() - 1
        return pl.BlockSpec((1, rows, width), lambda g, p: (p[2] >> shift, 0, 0))

    extra = [] if before is None else [before]
    block = pl.BlockSpec((rows, width), lambda g, p: (first + g, 0))
    return pl.pallas_call(
        body,
        grid_spec=pltpu.PrefetchScalarGridSpec(
            num_scalar_prefetch=1,
            grid=(count,),
            in_specs=[
                pl.BlockSpec(index.shape, lambda g, p: (0, 0)), block, *[own_block(a) for a in flat],
                *[pl.BlockSpec(memory_space=pl.ANY) for _ in extra],
            ],
            out_specs=block,
        ),
        out_shape=jax.ShapeDtypeStruct(error.shape, jnp.float32),
        input_output_aliases={} if before is None else {3 + len(flat): 0},
        name="error_step",
    )(place, index, error, *flat, *extra)


def weight_step(sets, groups, where, index, values, shape, momentum=None, before=None):
    count, subs = len(sets), len(sets[0])
    per = sets[0][0].shape[0]
    pieces = subs * per
    halves, _, islands, own_rows, width = shape
    cap = values.shape[3]
    tiles_row = width // TILE
    slots = islands * cap
    rate = outer_rate * (1.0 + outer_momentum) / islands
    flat = [a for one in sets for a in one]

    def body(w, ix, v, *refs):
        arrays, (held, sems) = refs[: len(flat)], refs[-2:]
        out = refs[-3] if momentum is None else refs[-4]
        step = pl.program_id(0)

        def copy(n):
            to = held.at[n // subs, pl.ds(n % subs * per, per)]
            return pltpu.make_async_copy(arrays[n], to, sems.at[n])

        @pl.when(step == 0)
        def _():
            for n in range(len(flat)):
                copy(n).start()

        for s in range(count):

            @pl.when(step == s)
            def _(s=s):
                for u in range(subs):
                    copy(s * subs + u).wait()

        owner = w[2 + step]
        for i in range(pieces):
            device = w[1] ^ groups[i]
            parts = block_delta(ix[device, owner], v[:, device, owner].reshape(slots, TILE), own_rows, tiles_row)
            to = device >> 1
            for c in range(tiles_row):
                at = slice(c * TILE, (c + 1) * TILE)
                part = parts[c * own_rows : (c + 1) * own_rows]
                if momentum is not None and groups[i] == 0:
                    refs[-3][:, at] = outer_momentum * refs[len(flat)][:, at] + part * (1.0 / islands)
                out[to, 0, 0, :, at] = (held[step, i, :, at].astype(jnp.float32) - rate * part).astype(jnp.bfloat16)

    extra = [v for v in (momentum, before) if v is not None]
    rows = pl.BlockSpec((own_rows, width), lambda g, w: (w[2 + g], 0))
    hbm = pl.BlockSpec(memory_space=pl.ANY)
    new_weight = jax.ShapeDtypeStruct(shape, jnp.bfloat16)
    block = pl.BlockSpec((halves, 1, 1, own_rows, width), lambda g, w: (0, w[0], w[2 + g], 0, 0))
    return pl.pallas_call(
        body,
        grid_spec=pltpu.PrefetchScalarGridSpec(
            num_scalar_prefetch=1,
            grid=(count,),
            in_specs=[
                pl.BlockSpec(index.shape, lambda g, w: (0, 0, 0, 0)),
                pl.BlockSpec(values.shape, lambda g, w: (0, 0, 0, 0, 0)),
                *[hbm for _ in flat],
                *([] if momentum is None else [rows]),
                *([] if before is None else [hbm]),
            ],
            out_specs=block if momentum is None else [block, rows],
            scratch_shapes=[
                pltpu.VMEM((count, pieces, own_rows, width), jnp.bfloat16),
                pltpu.SemaphoreType.DMA((len(flat),)),
            ],
        ),
        out_shape=new_weight if momentum is None else [new_weight, jax.ShapeDtypeStruct(momentum.shape, jnp.float32)],
        input_output_aliases={} if before is None else {2 + len(flat) + len(extra): 0},
        name="weight_step",
    )(where, index, values, *flat, *extra)


def local(inputs, grad_out, error, momentum, weight, tile_index):
    group = lax.axis_size("inside")
    islands = lax.axis_size("between")
    tokens, feat = inputs.shape
    width = grad_out.shape[1]
    rows_dev = feat // group
    own_rows = rows_dev // islands
    tiles_row = width // TILE
    own_tiles = own_rows * tiles_row
    cap = tile_index.shape[3]
    inside_bits = group.bit_length() - 1
    outer_bits = [*range(1, islands.bit_length() - 1), 0]
    chunks = max(1, min(4, rows_dev // TILE))
    rows = rows_dev // chunks
    halves = group // 2
    j = lax.axis_index("inside")
    b = lax.axis_index("between")
    place = jnp.stack([j & 1, (j >> 1) & 1, j])
    index = tile_index[0, 0]

    numbers = spread(index)
    island_numbers = numbers.reshape(group, 1, islands * cap)

    dy_recv = swap(grad_out, "inside", 0)
    x_send = take_halves(place, inputs, rows_dev, chunks)

    terms = slot_terms(place, inputs, grad_out, island_numbers, rows_dev, own_rows)
    terms, numbers = lax.optimization_barrier((terms, numbers))
    terms = lax.all_to_all(terms, "inside", split_axis=0, concat_axis=0, tiled=True)

    numbers = numbers[None]
    for bit in outer_bits:
        numbers = jnp.concatenate([numbers, swap(numbers, "between", bit)], axis=0)
    by_device = numbers.transpose(1, 2, 0, 3).reshape(group, islands, 1, islands * cap)

    start = b * own_rows
    base = (
        lax.dynamic_slice_in_dim(weight, start, own_rows, 0).astype(jnp.float32)
        - outer_rate * outer_momentum * outer_momentum * lax.dynamic_slice_in_dim(momentum, start, own_rows, 0)
    ).astype(jnp.bfloat16)[None]
    base_parts = []
    base_group = [0]
    for bit in reversed(range(1, inside_bits)):
        last = swap(base, "inside", bit)
        base_parts = [base, last]
        base = jnp.concatenate(base_parts, axis=0)
        base_group += [g ^ (1 << bit) for g in base_group]

    x_recv = []
    for k in range(chunks):
        x_recv.append(swap(x_send[k], "inside", 0))

    scale = 1.0 / math.sqrt(tokens * group)
    tiles = error[0].reshape(islands, own_tiles, TILE)
    picked = jnp.take_along_axis(tiles, jnp.maximum(index, 0)[:, :, None], axis=1)
    sums = jnp.sum(terms.astype(jnp.float32), axis=0).reshape(islands, cap, TILE)
    sent = jnp.where(index[:, :, None] >= 0, feedback_decay * picked + scale * sums, 0.0).astype(jnp.bfloat16)
    values = spread(sent)[None]
    for bit in outer_bits:
        values = jnp.concatenate([values, swap(values, "between", bit)], axis=0)

    across = []
    for part in base_parts:
        across.append(swap(part, "inside", 0))
    near_sets, far_sets = [[base]], [across]
    owners = [0]
    for bit in outer_bits:
        near_sets += swap_sets(near_sets, bit)
        far_sets += swap_sets(far_sets, bit)
        owners += [o ^ (1 << bit) for o in owners]
    set_owner = [b ^ o for o in owners]
    shape = (halves, 2, islands, own_rows, width)
    where = [jnp.stack([(j & 1) ^ parity, j, *set_owner]) for parity in range(2)]
    new_weight, new_momentum = weight_step(near_sets, base_group, where[0], by_device, values, shape, momentum)
    new_weight = weight_step(far_sets, [g ^ 1 for g in base_group], where[1], by_device, values, shape, None, new_weight)
    new_weight = new_weight.reshape(feat, width)

    parts = []
    for k in range(chunks):
        send, keep = pair_dot(place, inputs, x_recv[k], grad_out, dy_recv, k, chunks, halves)
        recv = swap(send, "inside", 1)
        terms = [keep, recv]
        for bit in range(2, inside_bits):
            current = (keep + recv.astype(jnp.float32)).reshape(keep.shape[0] // 2, 2, rows, width)
            mine = (j >> bit) & 1
            send = lax.dynamic_index_in_dim(current, 1 - mine, 1, keepdims=False).astype(jnp.bfloat16)
            keep = lax.dynamic_index_in_dim(current, mine, 1, keepdims=False)
            recv = swap(send, "inside", bit)
            terms.append(recv)
        parts.append(terms)
    flat_index = index.reshape(1, islands * cap)
    new_error = None
    cuts = sorted({0, min(1, chunks - 1), chunks - 1, chunks})
    for first, end in zip(cuts, cuts[1:]):
        new_error = error_step(place, parts[first:end], first, flat_index, error[0], own_rows, scale, new_error)
    new_error = new_error[None]
    return (new_weight, new_momentum, new_error)


def solution(mesh):
    in_specs = (
        P(("between", "inside"), None),
        P(("between", "inside"), None),
        P("between", "inside", None),
        P("inside", None),
        P("inside", None),
        P("between", "inside", None, None),
    )
    out_specs = (P(), P("inside", None), P("between", "inside", None))
    return jax.shard_map(local, mesh=mesh, in_specs=in_specs, out_specs=out_specs, check_vma=False)
```
